128 devices in a mesh: orb: 32 (over y, z, core), row: 4 (over x).
Axes of the slice: x: 4, y: 4, z: 4, core: 2. Of those that a mesh axis runs over, the one named last changes fastest.
Arguments:
- half_ints: bfloat16 [256, 2048, 1536], P(('orb', 'row')), may hold values from -0.125 to 0.125
- metric_inv: bfloat16 [128, 128, 128], P(('orb', 'row')), may hold values from -0.1 to 1.4, as said below
- coefficients: bfloat16 [4096, 256], P(('orb', 'row')), may hold values from -0.15625 to 0.15625
- basis_domain: int32 [256, 12], P(('orb', 'row')), may hold values from 0 to 31, as said below
- aux_domain: int32 [256, 16], P(('orb', 'row')), may hold values from 0 to 127, as said below
- aux_count: int32 [256], P(('orb', 'row')), may hold values from 8 to 16, as said below
Outputs:
- exchange_matrix: float32 [4096, 4096], P(('orb', 'row'))
- self_energy: float32 [], replicated
The draws below stay inside these ranges and needn't reach their ends.
Inputs may be any that keep to these rules, and one draw needn't show every extreme that they name: `metric_inv`: each block is lower triangular. `basis_domain`: each row names 12 different basis blocks. Among the 2 rows of one device (rows d * 2 to (d + 1) * 2 - 1), no basis block is named by more than 1 row (the two orbitals' domains are disjoint). `aux_domain`: each row names 16 different auxiliary blocks. Orbital i uses the first aux_count[i] blocks of its list; some orbital uses all 16.
All inputs are finite; a program needn't handle non-finite values.
Results may differ from the reference program's by a relative error of at most 0.00079.
Values may be sent and summed in bfloat16 or wider, within the bound.
A program may use at most 128 MiB of HBM per device.

```python
import jax
import jax.numpy as jnp
from jax import lax

BLK = 128
NBB = 32
NAB = 128
NBD = 12
NAD = 16
ORB_DEV = 2
NOCC = 256
NB = 4096


def distinct_blocks(key, row_count, picked, available):
    scores = jax.random.randint(key, (row_count, available), 0, 1048576) * available
    scores = scores + jnp.arange(available, dtype=jnp.int32)[None, :]
    ranking = jnp.argsort(scores, axis=1)
    return ranking[:, :picked].astype(jnp.int32)


def draw_basis_domain(key, part):
    groups = NOCC // ORB_DEV
    order = distinct_blocks(jax.random.fold_in(key, 11), groups, NBB, NBB)
    positions = (jnp.arange(ORB_DEV, dtype=jnp.int32)[:, None] * NBD + jnp.arange(NBD, dtype=jnp.int32)[None, :]) % NBB
    picked = order[:, positions.reshape(-1)]
    return picked.reshape(NOCC, NBD).astype(jnp.int32)


def draw_aux_domain(key, part):
    return distinct_blocks(jax.random.fold_in(key, 12), NOCC, NAD, NAB)


def draw_aux_count(key, part):
    subkeys = jax.random.split(jax.random.fold_in(key, 13), 3)
    half_count = NAD // 2
    draw_one = jax.random.randint(subkeys[0], (NOCC,), 0, NAD)
    draw_two = jax.random.randint(subkeys[1], (NOCC,), 0, NAD)
    counts = half_count + draw_one * draw_two * (NAD - half_count) // (NAD - 1) ** 2
    chosen = jax.random.randint(subkeys[2], (), 0, NOCC)
    return counts.at[chosen].set(NAD).astype(jnp.int32)


def draw_metric_inv(key, part):
    subkeys = jax.random.split(jax.random.fold_in(key, 14), 2)
    diagonal = jax.random.uniform(subkeys[0], (NAB, BLK), jnp.float32, 0.8, 1.2)
    strict_part = jax.random.uniform(subkeys[1], (NAB, BLK, BLK), jnp.float32, -0.099, 0.099)
    positions = jnp.arange(BLK)
    below_mask = (positions[:, None] > positions[None, :]).astype(jnp.float32)
    on_diagonal = (positions[:, None] == positions[None, :]).astype(jnp.float32)
    return (strict_part * below_mask + diagonal[:, :, None] * on_diagonal).astype(jnp.bfloat16)


def level_of(rng, shape, pieces, least, top_value):
    level = 1.0
    for axis_at, blocks in pieces:
        heights = jax.random.uniform(jax.random.fold_in(jax.random.fold_in(rng, 6), axis_at), (blocks,), jnp.float32, least / len(pieces), top_value / len(pieces))
        level = level * jnp.repeat(jnp.exp(heights), shape[axis_at] // blocks).reshape((-1,) + (1,) * (len(shape) - 1 - axis_at))
    return level


def centred(rng, extent, deviation, reach, shards=(), kind=jnp.bfloat16):
    array = deviation * jax.random.normal(rng, extent, jnp.float32)
    if shards:
        array = array * level_of(rng, extent, shards, -0.22, 0.18)
    return jnp.clip(array, -reach, reach).astype(kind)


def setup_inputs(seed: int = 0) -> dict:
    key_of = jax.random.split(jax.random.key(seed), 7)
    half_ints = centred(key_of[0], (NOCC, NAD * BLK, NBD * BLK), (NAD * BLK) ** -0.5, 0.125, ((0, 128),))
    metric_inv = draw_metric_inv(jax.random.fold_in(key_of[6], 71), 0)
    coefficients = centred(key_of[2], (NB, NOCC), (NBD * BLK) ** -0.5, 0.15625, ((0, 128),))
    basis_domain = draw_basis_domain(jax.random.fold_in(key_of[6], 71), 0)
    aux_domain = draw_aux_domain(jax.random.fold_in(key_of[6], 71), 0)
    aux_count = draw_aux_count(jax.random.fold_in(key_of[6], 71), 0)
    return {"half_ints": half_ints, "metric_inv": metric_inv, "coefficients": coefficients, "basis_domain": basis_domain, "aux_domain": aux_domain, "aux_count": aux_count}


def fit_orbital(block_rows, aux_ids, live_count, basis_ids, coef_column, metric_inv):
    block_width = metric_inv.shape[1]
    columns = block_rows.shape[1]
    group_size = min(4, NAD)
    coef_domain = coef_column.reshape(NBB, block_width)[basis_ids].reshape(-1).astype(jnp.float32)
    group_total = (live_count + group_size - 1) // group_size

    def advance(group_index, carry):
        k_partial, energy = carry
        first_block = group_index * group_size
        rows_now = lax.dynamic_slice_in_dim(block_rows, first_block * block_width, group_size * block_width, 0)
        rows_now = rows_now.astype(jnp.float32).reshape(group_size, block_width, columns)
        block_ids = lax.dynamic_slice_in_dim(aux_ids, first_block, group_size, 0)
        factors = metric_inv[block_ids].astype(jnp.float32)
        fitted = jnp.einsum("gqp,gpm->gqm", factors, rows_now, precision=lax.Precision.HIGHEST).astype(jnp.bfloat16)
        live_mask = (first_block + jnp.arange(group_size, dtype=jnp.int32)) < live_count
        fitted = jnp.where(live_mask[:, None, None], fitted, jnp.zeros_like(fitted))
        flat_rows = fitted.astype(jnp.float32).reshape(group_size * block_width, columns)
        k_partial = k_partial + jnp.dot(flat_rows.T, flat_rows, precision=lax.Precision.HIGHEST)
        projected = jnp.dot(flat_rows, coef_domain, precision=lax.Precision.HIGHEST)
        return k_partial, energy + jnp.sum(projected * projected)

    initial = (jnp.zeros((columns, columns), jnp.float32), jnp.zeros((), jnp.float32))
    return lax.fori_loop(0, group_total, advance, initial)


def reference(half_ints, metric_inv, coefficients, basis_domain, aux_domain, aux_count):
    block_width = metric_inv.shape[1]
    count_blocks = basis_domain.shape[1]

    def one_orbital(orbital, carry):
        k_whole, energy_sum = carry
        k_partial, energy = fit_orbital(half_ints[orbital], aux_domain[orbital], aux_count[orbital],
                                        basis_domain[orbital], coefficients[:, orbital], metric_inv)
        rounded = lax.optimization_barrier(k_partial.astype(jnp.bfloat16)).astype(jnp.float32)
        k_tiles = rounded.reshape(count_blocks, block_width, count_blocks, block_width).transpose(0, 2, 1, 3)
        block_ids = basis_domain[orbital]
        k_whole = k_whole.at[block_ids[:, None], :, block_ids[None, :], :].add(k_tiles)
        return k_whole, energy_sum + energy

    initial = (jnp.zeros((NBB, block_width, NBB, block_width), jnp.float32), jnp.zeros((), jnp.float32))
    k_whole, energy_sum = lax.fori_loop(0, NOCC, one_orbital, initial)
    return k_whole.reshape(NB, NB), energy_sum / NOCC
```

```python
import functools

import jax
import jax.numpy as jnp
from jax import lax
from jax.experimental import pallas as pl
from jax.experimental.pallas import tpu as pltpu
from jax.sharding import PartitionSpec as P

AXES = ("orb", "row")


def fit_kernel(shape, dom_ref, aux_ref, count_ref, half_ref, metric_ref, coef_ref, send_ref, energy_ref, fitted, coef_dom):
    orbs, aux_n, dom_n, width, span = shape
    step = pl.program_id(0)
    columns = dom_n * width
    fit_steps = orbs * aux_n

    @pl.when(step == 0)
    def _():
        energy_ref[...] = jnp.zeros_like(energy_ref)
        for orb in range(orbs):
            for k in range(dom_n):
                coef_dom[orb, :, k * width : (k + 1) * width] = coef_ref[orb, dom_ref[orb, k]]

    @pl.when(step < fit_steps)
    def _():
        orb = step // aux_n
        a = step % aux_n
        factor = metric_ref[aux_ref[orb, a]]
        block = jnp.dot(factor, half_ref[0], preferred_element_type=jnp.float32)
        block = jnp.where(a < count_ref[orb], block, 0.0).astype(jnp.bfloat16)
        rows = pl.ds(pl.multiple_of(a * width, width), width)
        fitted[orb, rows, 0:columns] = block
        fitted[orb, rows, columns:] = block[:, 0 : (span - 1) * width]
        weighted = block.astype(jnp.float32) * coef_dom[orb]
        projected = jnp.sum(weighted, axis=1, keepdims=True)
        energy_ref[...] += jnp.sum(projected * projected, axis=0, keepdims=True)

    @pl.when(step >= fit_steps)
    def _():
        orb = (step - fit_steps) // dom_n
        k = (step - fit_steps) % dom_n
        left = fitted[orb, :, pl.ds(pl.multiple_of(k * width, width), width)]
        right = fitted[orb, :, pl.ds(pl.multiple_of(k * width, width), span * width)]
        out = lax.dot_general(left, right, (((0,), (0,)), ((), ())), preferred_element_type=jnp.float32)
        send_ref[0] = out.astype(jnp.bfloat16)


def fit_rows(half_ints, metric_all, coef_blocks, basis_domain, aux_domain, aux_count, basis_blocks):
    orbs, aux_rows, columns = half_ints.shape
    width = metric_all.shape[1]
    aux_n, dom_n = aux_domain.shape[1], basis_domain.shape[1]
    span = dom_n // 2 + 1
    fit_steps = orbs * aux_n
    steps = fit_steps + orbs * dom_n

    def half_map(step, dom, aux, count):
        at = jnp.minimum(step, fit_steps - 1)
        return (at // aux_n, at % aux_n, 0)

    def send_map(step, dom, aux, count):
        at = jnp.maximum(step - fit_steps, 0)
        return (dom[at // dom_n, at % dom_n], 0, 0)

    return pl.pallas_call(
        functools.partial(fit_kernel, (orbs, aux_n, dom_n, width, span)),
        grid_spec=pltpu.PrefetchScalarGridSpec(
            num_scalar_prefetch=3,
            grid=(steps,),
            in_specs=[
                pl.BlockSpec((1, width, columns), half_map),
                pl.BlockSpec(memory_space=pltpu.VMEM),
                pl.BlockSpec(memory_space=pltpu.VMEM),
            ],
            out_specs=[
                pl.BlockSpec((1, width, span * width), send_map),
                pl.BlockSpec((1, 1), lambda step, dom, aux, count: (0, 0)),
            ],
            scratch_shapes=[
                pltpu.VMEM((orbs, aux_rows, columns + (span - 1) * width), jnp.bfloat16),
                pltpu.VMEM((orbs, 1, columns), jnp.float32),
            ],
        ),
        out_shape=[
            jax.ShapeDtypeStruct((basis_blocks, width, span * width), jnp.bfloat16),
            jax.ShapeDtypeStruct((1, 1), jnp.float32),
        ],
        compiler_params=pltpu.CompilerParams(
            vmem_limit_bytes=56 * 1024 * 1024, dimension_semantics=("arbitrary",)
        ),
        name="fit_rows",
    )(basis_domain, aux_domain, aux_count, half_ints, metric_all, coef_blocks)


def gather_rows_kernel(batch, span, half_last, ids_ref, arrived_ref, total_ref, turned_ref, acc):
    step = pl.program_id(0)
    blocks = acc.shape[0] - 1
    rows, width = acc.shape[1], acc.shape[2]
    quarters = width // rows

    @pl.when(step == 0)
    def _():
        acc[...] = jnp.zeros_like(acc)

    for s in range(batch):
        for j in range(span):
            where = ids_ref[step * batch + s, j]
            part = arrived_ref[s, :, j * width : (j + 1) * width].astype(jnp.float32)
            if j == 0 or (half_last and j == span - 1):
                part = part * 0.5
            acc[where] += part

    @pl.when(step == pl.num_programs(0) - 1)
    def _():
        for block in range(blocks):
            total_ref[:, block * width : (block + 1) * width] = acc[block]
        for group in range(blocks // quarters):
            tall = acc[group * quarters : (group + 1) * quarters].reshape(quarters * rows, width)
            turned = tall.T
            for beta in range(quarters):
                piece = turned[:, beta * rows : (beta + 1) * rows]
                for q in range(quarters):
                    tile = piece[q * rows : (q + 1) * rows]
                    packed = jnp.concatenate(
                        [tile[a * 8 : (a + 1) * 8] for a in range(rows // 8)], axis=1
                    )
                    turned_ref[(group * quarters + beta) * quarters + q] = packed


def gather_rows(ids, arrived, basis_blocks, half_last):
    devices, rows, columns = arrived.shape
    span = ids.shape[1]
    width = columns // span
    batch = 8
    return pl.pallas_call(
        functools.partial(gather_rows_kernel, batch, span, half_last),
        grid_spec=pltpu.PrefetchScalarGridSpec(
            num_scalar_prefetch=1,
            grid=(devices // batch,),
            in_specs=[pl.BlockSpec((batch, rows, columns), lambda step, ids: (step, 0, 0))],
            out_specs=[
                pl.BlockSpec((rows, basis_blocks * width), lambda step, ids: (0, 0)),
                pl.BlockSpec((devices, 8, width), lambda step, ids: (0, 0, 0)),
            ],
            scratch_shapes=[pltpu.VMEM((basis_blocks + 1, rows, width), jnp.float32)],
        ),
        out_shape=[
            jax.ShapeDtypeStruct((rows, basis_blocks * width), jnp.float32),
            jax.ShapeDtypeStruct((devices, 8, width), jnp.float32),
        ],
        compiler_params=pltpu.CompilerParams(dimension_semantics=("arbitrary",)),
        name="gather_rows",
    )(ids, arrived)


def finish_kernel(total_ref, tiles_ref, out_ref):
    rows, columns = total_ref.shape
    width = tiles_ref.shape[2]
    quarters = width // rows
    for block in range(columns // width):
        for a in range(rows // 8):
            strip = jnp.concatenate(
                [
                    tiles_ref[block * quarters + q, :, a * rows : (a + 1) * rows]
                    for q in range(quarters)
                ],
                axis=1,
            )
            at = slice(a * 8, (a + 1) * 8), slice(block * width, (block + 1) * width)
            out_ref[at] = total_ref[at] + strip


def finish(total, tiles):
    return pl.pallas_call(
        finish_kernel,
        out_shape=jax.ShapeDtypeStruct(total.shape, jnp.float32),
        name="finish",
    )(total, tiles)


def per_device(half_ints, metric_inv, coefficients, basis_domain, aux_domain, aux_count):
    devices = lax.axis_size(AXES)
    me = lax.axis_index(AXES)
    orbs = half_ints.shape[0]
    width = metric_inv.shape[1]
    rows = coefficients.shape[0]
    basis_blocks = rows * devices // width
    quarters = width // rows
    dom_n = basis_domain.shape[1]
    span = dom_n // 2 + 1

    metric_all = lax.all_gather(metric_inv, AXES, axis=0, tiled=True)
    coef_send = coefficients.T.reshape(devices, orbs * rows)
    dom_send = jnp.broadcast_to(
        basis_domain.reshape(1, orbs * dom_n).astype(jnp.bfloat16), (devices, orbs * dom_n)
    )
    small = jnp.concatenate([coef_send, dom_send], axis=1)
    small = lax.all_to_all(small, AXES, split_axis=0, concat_axis=0, tiled=True)
    coef_own = small[:, : orbs * rows].reshape(devices, orbs, rows).transpose(1, 0, 2)
    coef_blocks = coef_own.reshape(orbs, basis_blocks, 1, width).astype(jnp.float32)
    domains = small[:, orbs * rows :].astype(jnp.int32).reshape(devices, orbs, dom_n)

    send, energy = fit_rows(
        half_ints, metric_all, coef_blocks, basis_domain, aux_domain, aux_count, basis_blocks
    )
    arrived = lax.all_to_all(
        send.reshape(devices, rows, span * width), AXES, split_axis=0, concat_axis=0, tiled=True
    )
    energies = lax.all_to_all(
        jnp.broadcast_to(energy, (devices, 1)), AXES, split_axis=0, concat_axis=0, tiled=True
    )
    mine = me // quarters
    hits = (domains == mine).astype(jnp.int32)
    ids = jnp.stack(
        [jnp.sum(hits * (jnp.roll(domains, -j, axis=2) - basis_blocks), axis=(1, 2)) for j in range(span)],
        axis=1,
    ) + basis_blocks
    total, turned = gather_rows(ids, arrived, basis_blocks, dom_n % 2 == 0)
    tiles = lax.all_to_all(turned, AXES, split_axis=0, concat_axis=0, tiled=True)
    return finish(total, tiles), jnp.sum(energies) / (orbs * devices)


def solution(mesh):
    in_specs = (
        P(AXES, None, None),
        P(AXES, None, None),
        P(AXES, None),
        P(AXES, None),
        P(AXES, None),
        P(AXES),
    )
    out_specs = (P(AXES, None), P())
    return jax.shard_map(
        per_device, mesh=mesh, in_specs=in_specs, out_specs=out_specs, check_vma=False
    )
```

```python
import functools

import jax
import jax.numpy as jnp
from jax import lax
from jax.experimental import pallas as pl
from jax.experimental.pallas import tpu as pltpu
from jax.sharding import PartitionSpec as P

AXES = ("orb", "row")

MESH = pl.DeviceIdType.MESH


def spread_kernel(shape, parts, metric_ref, small_ref, all_ref, arrived_ref, part_send, part_recv, own_sem, small_sem):
    ny, nz, nc, nx = shape
    orb, x = lax.axis_index("orb"), lax.axis_index("row")
    c = lax.rem(orb, nc)
    z = lax.rem(orb // nc, nz)
    y = orb // (nc * nz)
    count = ny * nz * nc * nx
    me = orb * nx + x
    where = {"x": x, "y": y, "z": z}
    extent = {"x": nx, "y": ny, "z": nz}

    def device(y, z, c, x):
        return ((y * nz + z) * nc + c, x)

    def other(step):
        at = lax.rem(me + step, count)
        return at, (at // nx, lax.rem(at, nx))

    barrier = pltpu.get_barrier_semaphore()

    def greet(step, carry):
        pl.semaphore_signal(barrier, inc=1, device_id=other(step)[1], device_id_type=MESH)
        return carry

    lax.fori_loop(1, count, greet, 0)
    pl.semaphore_wait(barrier, count - 1)

    def region(gathered, rows):
        index = [pl.ds(0, extent[axis]) if axis in gathered else where[axis] for axis in ("y", "z")]
        last = pl.ds(0, nx) if "x" in gathered else x
        return all_ref.at[index[0], index[1], c, last, rows]

    orders = (("x", "y", "z"), ("y", "z", "x"), ("z", "x", "y"))
    own = pltpu.make_async_copy(metric_ref.at[0], all_ref.at[y, z, c, x], own_sem.at[0])
    own.start()
    started = []
    first = 0

    def ring(part, stage, rows):
        axis = orders[part][stage]
        copies = []
        for step in (2, 1, 3):
            at = dict(where)
            at[axis] = lax.rem(where[axis] + step, extent[axis])
            target = region(orders[part][:stage], rows)
            source = metric_ref.at[0, rows] if stage == 0 else target
            copies.append(
                pltpu.make_async_remote_copy(
                    src_ref=source,
                    dst_ref=target,
                    send_sem=part_send.at[part, stage, step - 1],
                    recv_sem=part_recv.at[part, stage, step - 1],
                    device_id=device(at["y"], at["z"], c, at["x"]),
                    device_id_type=MESH,
                )
            )
        return copies

    rows_of = []
    for part in range(3):
        rows_of.append(pl.ds(first, parts[part]))
        first += parts[part]
    flying = []
    for part in range(3):
        flying.append(ring(part, 0, rows_of[part]))
        for copy in flying[part]:
            copy.start()
        started += flying[part]

    def send_small(step, carry):
        at, target = other(step)
        pltpu.make_async_remote_copy(
            src_ref=small_ref.at[at],
            dst_ref=arrived_ref.at[me],
            send_sem=small_sem.at[0],
            recv_sem=small_sem.at[1],
            device_id=target,
            device_id_type=MESH,
        ).start()
        return carry

    lax.fori_loop(1, count, send_small, 0)
    own_small = pltpu.make_async_copy(small_ref.at[me], arrived_ref.at[me], own_sem.at[1])
    own_small.start()
    own.wait()

    for stage in range(1, 4):
        for part in range(3):
            for copy in flying[part]:
                copy.wait_recv()
            if stage < 3:
                flying[part] = ring(part, stage, rows_of[part])
            else:
                target = region(("x", "y", "z"), rows_of[part])
                flying[part] = [
                    pltpu.make_async_remote_copy(
                        src_ref=target,
                        dst_ref=target,
                        send_sem=part_send.at[part, 3, 0],
                        recv_sem=part_recv.at[part, 3, 0],
                        device_id=device(y, z, 1 - c, x),
                        device_id_type=MESH,
                    )
                ]
            for copy in flying[part]:
                copy.start()
            started += flying[part]
    for part in range(3):
        for copy in flying[part]:
            copy.wait_recv()
    for copy in started:
        copy.wait_send()
    own_small.wait()
    pltpu.make_async_remote_copy(
        src_ref=small_ref.at[pl.ds(0, count - 1)],
        dst_ref=arrived_ref.at[pl.ds(0, count - 1)],
        send_sem=small_sem.at[0],
        recv_sem=small_sem.at[1],
        device_id=other(1)[1],
        device_id_type=MESH,
    ).wait()


def spread(metric_inv, small, shape):
    width = metric_inv.shape[1]
    third = (width // 3 + 15) // 16 * 16
    return pl.pallas_call(
        functools.partial(spread_kernel, shape, (third, third, width - 2 * third)),
        in_specs=[pl.BlockSpec(memory_space=pltpu.VMEM)] * 2,
        out_specs=[pl.BlockSpec(memory_space=pltpu.VMEM)] * 2,
        out_shape=[
            jax.ShapeDtypeStruct(shape + metric_inv.shape[1:], metric_inv.dtype),
            jax.ShapeDtypeStruct(small.shape, small.dtype),
        ],
        scratch_shapes=[
            pltpu.SemaphoreType.DMA((3, 4, 3)),
            pltpu.SemaphoreType.DMA((3, 4, 3)),
            pltpu.SemaphoreType.DMA((2,)),
            pltpu.SemaphoreType.DMA((2,)),
        ],
        compiler_params=pltpu.CompilerParams(collective_id=0, has_side_effects=True),
        name="spread",
    )(metric_inv, small)


def exchange_kernel(
    shape, dom_ref, aux_ref, row_ref, live_ref, half_ref, metric_ref, small_ref, arrived_ref, energy_ref,
    fitted, coef_dom, stage, send_sem, recv_sem, own_sem,
):
    orbs, aux_n, dom_n, width, span, group, blocks, quarters, torus = shape
    step = pl.program_id(0)
    columns = dom_n * width
    rows = width // quarters
    count = blocks * quarters
    fit_steps = orbs * aux_n // group
    window = dom_n + span - 1
    ny, nz, nc = torus
    orb_at, x = lax.axis_index("orb"), lax.axis_index("row")
    me = orb_at * quarters + x
    c = lax.rem(orb_at, nc)
    z = lax.rem(orb_at // nc, nz)
    y = orb_at // (nc * nz)
    barrier = pltpu.get_barrier_semaphore()

    @pl.when(step == 0)
    def _():
        def greet(i, carry):
            at = lax.rem(me + i, count)
            pl.semaphore_signal(
                barrier, inc=1, device_id=(at // quarters, lax.rem(at, quarters)), device_id_type=MESH
            )
            return carry

        lax.fori_loop(1, count, greet, 0)
        energy_ref[...] = jnp.zeros_like(energy_ref)
        for orb in range(orbs):
            for k in range(dom_n):
                pieces = [
                    small_ref[dom_ref[orb, k] * quarters + q][:, orb * rows : (orb + 1) * rows]
                    for q in range(quarters)
                ]
                coef_dom[orb, :, k * width : (k + 1) * width] = jnp.concatenate(pieces, axis=1)

    @pl.when(step < fit_steps)
    def _():
        orb = step * group // aux_n
        first = step * group % aux_n
        energy = jnp.zeros((1, 1), jnp.float32)
        for g in range(group):
            a = first + g
            factor = metric_ref[aux_ref[orb, a]]
            block = jnp.dot(
                factor, half_ref[0, g * width : (g + 1) * width], preferred_element_type=jnp.float32
            )
            block = (block * live_ref[orb * aux_n + a][:, 0:1]).astype(jnp.bfloat16)
            at = pl.ds(pl.multiple_of(a * width, width), width)
            for j in range(window):
                k = j % dom_n
                fitted[orb * window + j, at] = block[:, k * width : (k + 1) * width]
            weighted = block.astype(jnp.float32) * coef_dom[orb]
            projected = jnp.sum(weighted, axis=1, keepdims=True)
            energy += jnp.sum(projected * projected, axis=0, keepdims=True)
        energy_ref[...] += jnp.broadcast_to(energy, energy_ref.shape)

    @pl.when(step == fit_steps)
    def _():
        pl.semaphore_wait(barrier, count - 1)

    def target(i):
        ty = lax.rem(y + i, ny)
        tz = lax.rem(z + i + i // ny, nz)
        tc = lax.rem(c + i // (ny * nz), nc)
        return (ty * nz + tz) * nc + tc

    @pl.when(step > fit_steps)
    def _():
        i = step - fit_steps - 1
        block = target(i)
        for q in range(quarters):
            part = stage.at[i, q * rows : (q + 1) * rows]
            here = jnp.logical_and(block == orb_at, x == q)

            @pl.when(here)
            def _():
                pltpu.make_async_copy(part, arrived_ref.at[me], own_sem).start()

            @pl.when(jnp.logical_not(here))
            def _():
                pltpu.make_async_remote_copy(
                    src_ref=part,
                    dst_ref=arrived_ref.at[me],
                    send_sem=send_sem,
                    recv_sem=recv_sem,
                    device_id=(block, q),
                    device_id_type=MESH,
                ).start()

    @pl.when(jnp.logical_and(step >= fit_steps, step < fit_steps + blocks))
    def _():
        i = step - fit_steps
        block = target(i)
        first = row_ref[block]
        left = fitted[first]
        right = jnp.concatenate([fitted[first + j] for j in range(span)], axis=1)
        out = lax.dot_general(left, right, (((0,), (0,)), ((), ())), preferred_element_type=jnp.float32)
        stage[i] = out.astype(jnp.bfloat16)

    @pl.when(step == fit_steps + blocks)
    def _():
        pltpu.make_async_copy(stage.at[0, 0:rows], arrived_ref.at[me], own_sem).wait()
        others = arrived_ref.at[pl.ds(0, count - 1)]
        pltpu.make_async_remote_copy(
            src_ref=others,
            dst_ref=others,
            send_sem=send_sem,
            recv_sem=recv_sem,
            device_id=(lax.rem(orb_at + 1, blocks), x),
            device_id_type=MESH,
        ).wait()


def exchange(half_ints, metric_all, small, basis_domain, aux_domain, aux_count, basis_blocks, torus):
    orbs, aux_rows, columns = half_ints.shape
    devices, width = metric_all.shape[:2]
    aux_n, dom_n = aux_domain.shape[1], basis_domain.shape[1]
    span = dom_n // 2 + 1
    group = 4
    quarters = devices // basis_blocks
    rows = width // quarters
    fit_steps = orbs * aux_n // group
    per_orb = aux_n // group

    def half_map(step):
        at = jnp.minimum(step, fit_steps - 1)
        return (at // per_orb, at % per_orb, 0)

    window = dom_n + span - 1
    start = jnp.arange(orbs * dom_n, dtype=jnp.int32)
    start = start // dom_n * window + start % dom_n
    block_ids = jnp.arange(basis_blocks, dtype=jnp.int32)
    found = basis_domain.reshape(1, orbs * dom_n) == block_ids[:, None]
    row_at = jnp.sum(jnp.where(found, start[None], 0), axis=1)
    live = jnp.arange(aux_n, dtype=jnp.int32)[None, :] < aux_count[:, None]
    live = jnp.broadcast_to(live.astype(jnp.float32).reshape(orbs * aux_n, 1, 1), (orbs * aux_n, 1, width))
    vmem = pl.BlockSpec(memory_space=pltpu.VMEM)
    smem = pl.BlockSpec(memory_space=pltpu.SMEM)
    return pl.pallas_call(
        functools.partial(
            exchange_kernel, (orbs, aux_n, dom_n, width, span, group, basis_blocks, quarters, torus)
        ),
        grid=(fit_steps + basis_blocks + 1,),
        in_specs=[smem, smem, smem, vmem, pl.BlockSpec((1, group * width, columns), half_map), vmem, vmem],
        out_specs=[pl.BlockSpec(memory_space=pl.ANY), pl.BlockSpec((1, width), lambda step: (0, 0))],
        out_shape=[
            jax.ShapeDtypeStruct((devices, rows, span * width), jnp.bfloat16),
            jax.ShapeDtypeStruct((1, width), jnp.float32),
        ],
        scratch_shapes=[
            pltpu.VMEM((orbs * window, aux_rows, width), jnp.bfloat16),
            pltpu.VMEM((orbs, 1, columns), jnp.float32),
            pltpu.VMEM((basis_blocks, width, span * width), jnp.bfloat16),
            pltpu.SemaphoreType.DMA,
            pltpu.SemaphoreType.DMA,
            pltpu.SemaphoreType.DMA,
        ],
        compiler_params=pltpu.CompilerParams(
            collective_id=1,
            has_side_effects=True,
            vmem_limit_bytes=60 * 1024 * 1024,
            dimension_semantics=("arbitrary",),
        ),
        name="exchange",
    )(basis_domain, aux_domain, row_at, live, half_ints, metric_all, small)


def gather_rows_kernel(batch, span, half_last, ids_ref, arrived_ref, total_ref, turned_ref, acc):
    step = pl.program_id(0)
    blocks = acc.shape[0] - 1
    rows, width = acc.shape[1], acc.shape[2]
    quarters = width // rows

    @pl.when(step == 0)
    def _():
        acc[...] = jnp.zeros_like(acc)

    for s in range(batch):
        places = [ids_ref[step * batch + s, j] for j in range(span)]
        sums = []
        for j in range(span):
            part = arrived_ref[s, :, j * width : (j + 1) * width].astype(jnp.float32)
            if j == 0 or (half_last and j == span - 1):
                part = part * 0.5
            sums.append(acc[places[j]] + part)
        for j in range(span):
            acc[places[j]] = sums[j]

    @pl.when(step == pl.num_programs(0) - 1)
    def _():
        for block in range(blocks):
            total_ref[:, block * width : (block + 1) * width] = acc[block]
        for group in range(blocks // quarters):
            tall = acc[group * quarters : (group + 1) * quarters].reshape(quarters * rows, width)
            turned = tall.T
            for beta in range(quarters):
                piece = turned[:, beta * rows : (beta + 1) * rows]
                for q in range(quarters):
                    tile = piece[q * rows : (q + 1) * rows]
                    packed = jnp.concatenate(
                        [tile[a * 8 : (a + 1) * 8] for a in range(rows // 8)], axis=1
                    )
                    turned_ref[(group * quarters + beta) * quarters + q] = packed


def gather_rows(ids, arrived, basis_blocks, half_last):
    devices, rows, columns = arrived.shape
    span = ids.shape[1]
    width = columns // span
    batch = 8
    return pl.pallas_call(
        functools.partial(gather_rows_kernel, batch, span, half_last),
        grid_spec=pltpu.PrefetchScalarGridSpec(
            num_scalar_prefetch=1,
            grid=(devices // batch,),
            in_specs=[pl.BlockSpec((batch, rows, columns), lambda step, ids: (step, 0, 0))],
            out_specs=[
                pl.BlockSpec((rows, basis_blocks * width), lambda step, ids: (0, 0)),
                pl.BlockSpec((devices, 8, width), lambda step, ids: (0, 0, 0)),
            ],
            scratch_shapes=[pltpu.VMEM((basis_blocks + 1, rows, width), jnp.float32)],
        ),
        out_shape=[
            jax.ShapeDtypeStruct((rows, basis_blocks * width), jnp.float32),
            jax.ShapeDtypeStruct((devices, 8, width), jnp.float32),
        ],
        compiler_params=pltpu.CompilerParams(dimension_semantics=("arbitrary",)),
        name="gather_rows",
    )(ids, arrived)


def finish_kernel(quarters, total_ref, turned_ref, energy_ref, out_ref, mean_ref, tiles, energies, sems, own_sems):
    rows, columns = total_ref.shape
    width = turned_ref.shape[2]
    count = turned_ref.shape[0]
    me = lax.axis_index("orb") * quarters + lax.axis_index("row")

    def other(step):
        at = lax.rem(me + step, count)
        return at, (at // quarters, lax.rem(at, quarters))

    barrier = pltpu.get_barrier_semaphore()

    def greet(step, carry):
        pl.semaphore_signal(barrier, inc=1, device_id=other(step)[1], device_id_type=MESH)
        return carry

    lax.fori_loop(1, count, greet, 0)
    pl.semaphore_wait(barrier, count - 1)
    own = [
        pltpu.make_async_copy(turned_ref.at[me], tiles.at[me], own_sems.at[0]),
        pltpu.make_async_copy(energy_ref, energies.at[me], own_sems.at[1]),
    ]
    for copy in own:
        copy.start()

    def send(step, carry):
        at, device = other(step)
        pltpu.make_async_remote_copy(
            src_ref=turned_ref.at[at],
            dst_ref=tiles.at[me],
            send_sem=sems.at[0],
            recv_sem=sems.at[1],
            device_id=device,
            device_id_type=MESH,
        ).start()
        pltpu.make_async_remote_copy(
            src_ref=energy_ref,
            dst_ref=energies.at[me],
            send_sem=sems.at[2],
            recv_sem=sems.at[3],
            device_id=device,
            device_id_type=MESH,
        ).start()
        return carry

    lax.fori_loop(1, count, send, 0)
    for copy in own:
        copy.wait()
    for k, ref in enumerate((tiles, energies)):
        part = ref.at[pl.ds(0, count - 1)]
        pltpu.make_async_remote_copy(
            src_ref=part,
            dst_ref=part,
            send_sem=sems.at[2 * k],
            recv_sem=sems.at[2 * k + 1],
            device_id=other(1)[1],
            device_id_type=MESH,
        ).wait()
    for block in range(columns // width):
        for a in range(rows // 8):
            strip = jnp.concatenate(
                [tiles[block * quarters + q, :, a * rows : (a + 1) * rows] for q in range(quarters)],
                axis=1,
            )
            at = slice(a * 8, (a + 1) * 8), slice(block * width, (block + 1) * width)
            out_ref[at] = total_ref[at] + strip
    mean_ref[...] = jnp.sum(energies[...], axis=0)


def finish(total, turned, energy, quarters):
    devices, _, width = turned.shape
    return pl.pallas_call(
        functools.partial(finish_kernel, quarters),
        in_specs=[pl.BlockSpec(memory_space=pltpu.VMEM)] * 3,
        out_specs=[pl.BlockSpec(memory_space=pltpu.VMEM)] * 2,
        out_shape=[
            jax.ShapeDtypeStruct(total.shape, jnp.float32),
            jax.ShapeDtypeStruct((1, width), jnp.float32),
        ],
        scratch_shapes=[
            pltpu.VMEM(turned.shape, jnp.float32),
            pltpu.VMEM((devices, 1, width), jnp.float32),
            pltpu.SemaphoreType.DMA((4,)),
            pltpu.SemaphoreType.DMA((2,)),
        ],
        compiler_params=pltpu.CompilerParams(collective_id=2, has_side_effects=True),
        name="finish",
    )(total, turned, energy)


def per_device(half_ints, metric_inv, coefficients, basis_domain, aux_domain, aux_count):
    devices = lax.axis_size(AXES)
    me = lax.axis_index(AXES)
    orbs = half_ints.shape[0]
    width = metric_inv.shape[1]
    rows = coefficients.shape[0]
    basis_blocks = rows * devices // width
    quarters = width // rows
    dom_n = basis_domain.shape[1]
    span = dom_n // 2 + 1

    coef_send = coefficients.T.reshape(devices, orbs * rows).astype(jnp.float32)
    dom_send = jnp.broadcast_to(
        basis_domain.reshape(1, orbs * dom_n).astype(jnp.float32), (devices, orbs * dom_n)
    )
    small = jnp.concatenate([coef_send, dom_send], axis=1)
    small = jnp.pad(small, ((0, 0), (0, width - small.shape[1]))).reshape(devices, 1, width)
    torus = (4, 4, 2)
    metric_all, small = spread(metric_inv, small, torus + (quarters,))
    metric_all = metric_all.reshape(devices, width, width)
    arrived, energy = exchange(
        half_ints, metric_all, small, basis_domain, aux_domain, aux_count, basis_blocks, torus
    )
    domains = small[:, 0, orbs * rows : orbs * (rows + dom_n)].astype(jnp.int32)
    place = jnp.arange(orbs * dom_n, dtype=jnp.int32)[None, :]
    hits = domains == me // quarters
    at = jnp.sum(jnp.where(hits, place + 1, 0), axis=1) - 1
    turn = jnp.arange(span, dtype=jnp.int32)[None, :]
    wanted = jnp.where(at[:, None] < 0, -1, at[:, None] // dom_n * dom_n + (at[:, None] + turn) % dom_n)
    picked = wanted[:, :, None] == place[None]
    ids = jnp.sum(jnp.where(picked, domains[:, None, :] - basis_blocks, 0), axis=2) + basis_blocks
    total, turned = gather_rows(ids, arrived, basis_blocks, dom_n % 2 == 0)
    out, mean = finish(total, turned, energy, quarters)
    return out, mean[0, 0] / (orbs * devices)


def solution(mesh):
    in_specs = (
        P(AXES, None, None),
        P(AXES, None, None),
        P(AXES, None),
        P(AXES, None),
        P(AXES, None),
        P(AXES),
    )
    out_specs = (P(AXES, None), P())
    return jax.shard_map(
        per_device, mesh=mesh, in_specs=in_specs, out_specs=out_specs, check_vma=False
    )
```
